32 devices in a mesh: group: 2 (over x), frame: 4 (over y, core), row: 4 (over z).
Axes of the slice: x: 2, y: 2, z: 4, core: 2. Of those that a mesh axis runs over, the one named last changes fastest.
Arguments:
- latents: bfloat16 [48, 8, 64, 320], P(('group', 'frame'), 'row'), parts along dimension 0, may hold values from -8 to 8
- condition: bfloat16 [24, 8, 64, 320], P(('group', 'frame'), 'row'), parts along dimension 0, may hold values from -6 to 6
- key_frames: int32 [24], P('group'), parts along dimension 0, may hold values from -1 to 23, as said below
- propagate: int32 [48], P('group'), parts along dimension 0, may hold values from 0 to 11, as said below
- encoder_conv: bfloat16 [9, 320, 320], replicated, may hold values from -0.109375 to 0.109375
- zero_conv: bfloat16 [320, 320], replicated, may hold values from -0.3125 to 0.3125
- attention_gain: float32 [320], replicated, may hold values from 0.25 to 1.75
- query_weight: bfloat16 [320, 320], replicated, may hold values from -3 to 3
- key_weight: bfloat16 [320, 320], replicated, may hold values from -3 to 3
- value_weight: bfloat16 [320, 320], replicated, may hold values from -0.3125 to 0.3125
- output_weight: bfloat16 [320, 320], replicated, may hold values from -0.3125 to 0.3125
- conv_gain: float32 [320], replicated, may hold values from 0.25 to 1.75
- block_conv: bfloat16 [9, 320, 320], replicated, may hold values from -0.109375 to 0.109375
Outputs:
- updated: bfloat16 [48, 8, 64, 320], P(('group', 'frame'), 'row'), parts along dimension 0
The draws below stay inside these ranges and needn't reach their ends.
There are 2 independent parts, one for each index of `group`. The reference program is written for one: setup_inputs(seed, part) draws one part's arguments, and reference() takes and returns one part's arrays. A program takes and returns all parts, laid end to end along the dimension named above; an argument that names none is the same for every part. Nothing has to cross between parts.
Inputs may be any that keep to these rules, and one draw needn't show every extreme that they name: `key_frames`: the 3 slots of index d of frame hold keyframes of frames d * 6 to (d + 1) * 6 - 1, all different, live slots first; of index d and the index half the frame axis away, one holds 3 live keyframes and the other 1. `propagate`: each frame names a live slot of its own index of frame or of an adjacent one (no wrap); a keyframe's own frame names its own slot.
All inputs are finite; a program needn't handle non-finite values.
Results may differ from the reference program's by a relative error of at most 0.014.
Values may be sent and summed in bfloat16 or wider, within the bound.
A program may use at most 64 MiB of HBM per device.

```python
import math
import jax
import jax.numpy as jnp
from jax import lax

C = 320
HEADS = 8
WIDTH = 64
FRAMES_DEV = 6
KEY_LOW = 1
KEY_SLOTS = 3
FRAMES = 24
HEIGHT = 8
KEYS = 12
N_FRAME = 4


def plan_keys(key):
    seeded = jax.random.fold_in(key, 7)
    key_busy, key_perm, key_side, key_pick = jax.random.split(seeded, 4)
    pair_count = N_FRAME // 2
    devices = jnp.arange(N_FRAME, dtype=jnp.int32)
    coin_flip = jax.random.randint(key_busy, (pair_count,), 0, 2)
    lower_half = devices < pair_count
    partner_coin = coin_flip[devices % pair_count]
    crowded = jnp.where(lower_half, partner_coin == 1, partner_coin == 0)
    live_count = jnp.where(crowded, 3 * KEY_LOW, KEY_LOW).astype(jnp.int32)
    orders = jax.vmap(lambda subkey: jax.random.permutation(subkey, FRAMES_DEV))(jax.random.split(key_perm, N_FRAME)).astype(jnp.int32)
    slot_ids = jnp.arange(KEY_SLOTS, dtype=jnp.int32)
    is_live = slot_ids[None, :] < live_count[:, None]
    key_frames = jnp.where(is_live, devices[:, None] * FRAMES_DEV + orders[:, :KEY_SLOTS], -1).reshape(-1)
    ranks_row = jnp.broadcast_to(jnp.arange(FRAMES_DEV, dtype=jnp.int32)[None, :], (N_FRAME, FRAMES_DEV))
    frame_rank = jnp.zeros((N_FRAME, FRAMES_DEV), jnp.int32).at[jnp.broadcast_to(devices[:, None], (N_FRAME, FRAMES_DEV)), orders].set(ranks_row)
    is_key = frame_rank < live_count[:, None]
    offset_side = jax.random.randint(key_side, (N_FRAME, FRAMES_DEV), -1, 2)
    offset_side = jnp.where(frame_rank == KEY_SLOTS, -1, offset_side)
    offset_side = jnp.where(frame_rank == KEY_SLOTS + 1, 1, offset_side)
    target = jnp.clip(devices[:, None] + offset_side, 0, N_FRAME - 1)
    slot_pick = jax.random.randint(key_pick, (N_FRAME, FRAMES_DEV), 0, 3 * KEY_LOW) % live_count[target]
    propagate = jnp.where(is_key, devices[:, None] * KEY_SLOTS + frame_rank, target * KEY_SLOTS + slot_pick).reshape(-1)
    return (key_frames.astype(jnp.int32), propagate.astype(jnp.int32))


def draw_key_frames(key, part):
    return plan_keys(key)[0]


def draw_propagate(key, part):
    return plan_keys(key)[1]


def draw_latents(key, part):
    full_shape = (FRAMES, HEIGHT, WIDTH, C)
    drawn = jax.random.normal(jax.random.fold_in(key, 33), full_shape, jnp.float32)
    return jnp.clip(drawn, -8.0, 8.0).astype(jnp.bfloat16)


def query_key_pair(key):
    first_weights = jax.random.normal(jax.random.fold_in(key, 43), (C, C), jnp.float32) / math.sqrt(C)
    second_weights = jax.random.normal(jax.random.fold_in(key, 44), (C, C), jnp.float32) / math.sqrt(C)
    return (jnp.clip(first_weights, -3.0, 3.0), jnp.clip(second_weights, -3.0, 3.0))


def draw_query_weight(key, part):
    return query_key_pair(key)[0].astype(jnp.bfloat16)


def draw_key_weight(key, part):
    return query_key_pair(key)[1].astype(jnp.bfloat16)


def level_of(stream_key, dims, shards, low, high):
    level = 1.0
    for position, blocks in shards:
        steps = jax.random.uniform(jax.random.fold_in(jax.random.fold_in(stream_key, 6), position), (blocks,), jnp.float32, low / len(shards), high / len(shards))
        level = level * jnp.repeat(jnp.exp(steps), dims[position] // blocks).reshape((-1,) + (1,) * (len(dims) - 1 - position))
    return level


def normal_values(own_key, shape, spread, bound, pieces=(), kind=jnp.bfloat16):
    level = level_of(own_key, shape, pieces, -0.22, 0.18) if pieces else 1.0
    array = jax.random.normal(own_key, shape, jnp.float32) * spread * level
    return jnp.minimum(jnp.maximum(array, -bound), bound).astype(kind)


def setup_inputs(seed: int = 0, part: int = 0) -> dict:
    streams_of = jax.random.split(jax.random.key(seed), 14)
    part_keys = jax.random.split(jax.random.fold_in(streams_of[13], part), 14)
    latents = draw_latents(jax.random.fold_in(jax.random.fold_in(streams_of[13], part), 71), part)
    condition = normal_values(part_keys[1], (KEYS, HEIGHT, WIDTH, C), 1.0, 6.0, ((0, 4), (1, 4)))
    key_frames = draw_key_frames(jax.random.fold_in(jax.random.fold_in(streams_of[13], part), 71), part)
    propagate = draw_propagate(jax.random.fold_in(jax.random.fold_in(streams_of[13], part), 71), part)
    encoder_conv = normal_values(streams_of[4], (9, C, C), (9 * C) ** -0.5, 0.109375)
    zero_conv = normal_values(streams_of[5], (C, C), C ** -0.5, 0.3125)
    attention_gain = jnp.clip(1.0 + 0.15 * jax.random.normal(streams_of[6], (C,), jnp.float32), 0.25, 1.75)
    query_weight = draw_query_weight(jax.random.fold_in(streams_of[13], 71), part)
    key_weight = draw_key_weight(jax.random.fold_in(streams_of[13], 71), part)
    value_weight = normal_values(streams_of[9], (C, C), C ** -0.5, 0.3125)
    output_weight = normal_values(streams_of[10], (C, C), C ** -0.5, 0.3125)
    conv_gain = jnp.clip(1.0 + 0.15 * jax.random.normal(streams_of[11], (C,), jnp.float32), 0.25, 1.75)
    block_conv = normal_values(streams_of[12], (9, C, C), (9 * C) ** -0.5, 0.109375)
    return {"latents": latents, "condition": condition, "key_frames": key_frames, "propagate": propagate, "encoder_conv": encoder_conv, "zero_conv": zero_conv, "attention_gain": attention_gain, "query_weight": query_weight, "key_weight": key_weight, "value_weight": value_weight, "output_weight": output_weight, "conv_gain": conv_gain, "block_conv": block_conv}


def convolve(images, weights):
    frame_count, row_count, col_count, channels = images.shape
    padded = jnp.pad(images, ((0, 0), (1, 1), (1, 1), (0, 0)))
    running = jnp.zeros((frame_count * row_count * col_count, weights.shape[2]), jnp.float32)
    for row_off in range(3):
        for col_off in range(3):
            window = padded[:, row_off:row_off + row_count, col_off:col_off + col_count, :].reshape(-1, channels)
            running = running + jnp.dot(window, weights[3 * row_off + col_off], preferred_element_type=jnp.float32)
    return running.reshape(frame_count, row_count, col_count, -1)

def layer_norm(values_in, scale_gain):
    average = lax.optimization_barrier(jnp.mean(values_in, axis=-1, keepdims=True))
    centered = values_in - average
    variance = lax.optimization_barrier(jnp.mean(centered * centered, axis=-1, keepdims=True))
    return centered * lax.rsqrt(variance + 1e-05) * scale_gain

def positions(frame_total, channels):
    frame_pos = jnp.arange(frame_total, dtype=jnp.float32)[:, None]
    half_index = jnp.arange(channels // 2, dtype=jnp.float32)
    frequency = jnp.exp(half_index * (-2.0 * math.log(10000.0) / channels))
    angles = frame_pos * frequency
    return jnp.stack([jnp.sin(angles), jnp.cos(angles)], axis=-1).reshape(frame_total, channels)

def reference(latents, condition, key_frames, propagate, encoder_conv, zero_conv, attention_gain, query_weight, key_weight, value_weight, output_weight, conv_gain, block_conv):
    encoded = lax.map(lambda single: jax.nn.silu(convolve(single[None], encoder_conv)[0]).astype(jnp.bfloat16), condition)
    keyres = jnp.dot(encoded.reshape(-1, C), zero_conv, preferred_element_type=jnp.float32).astype(jnp.bfloat16).reshape(encoded.shape)
    frame_ids = jnp.arange(FRAMES, dtype=jnp.int32)
    source_frame = key_frames[propagate]
    reach = jnp.exp(-jnp.abs(frame_ids - source_frame).astype(jnp.float32) / (2 * FRAMES_DEV))
    hidden = (latents.astype(jnp.float32) + reach[:, None, None, None] * keyres[propagate].astype(jnp.float32)).astype(jnp.bfloat16)
    encoding = positions(FRAMES, C)

    def attend_row(row_data):
        normed = (layer_norm(row_data.astype(jnp.float32), attention_gain) + encoding[:, None, :]).astype(jnp.bfloat16)
        flattened = normed.reshape(-1, C)
        head_shape = (FRAMES, WIDTH, HEADS, C // HEADS)
        query = jnp.dot(flattened, query_weight, preferred_element_type=jnp.float32).astype(jnp.bfloat16).reshape(head_shape)
        key_proj = jnp.dot(flattened, key_weight, preferred_element_type=jnp.float32).astype(jnp.bfloat16).reshape(head_shape)
        value_proj = jnp.dot(flattened, value_weight, preferred_element_type=jnp.float32).astype(jnp.bfloat16).reshape(head_shape)
        scores = jnp.einsum('fwhd,gwhd->whfg', query.astype(jnp.float32), key_proj.astype(jnp.float32)) / math.sqrt(C // HEADS)
        weights_soft = jax.nn.softmax(scores, axis=-1).astype(jnp.bfloat16)
        mixed_heads = jnp.einsum('whfg,gwhd->fwhd', weights_soft.astype(jnp.float32), value_proj.astype(jnp.float32)).astype(jnp.bfloat16).reshape(-1, C)
        projected = jnp.dot(mixed_heads, output_weight, preferred_element_type=jnp.float32)
        return (row_data.astype(jnp.float32).reshape(-1, C) + projected).astype(jnp.bfloat16).reshape(FRAMES, WIDTH, C)
    attended = jnp.moveaxis(lax.map(attend_row, jnp.moveaxis(hidden, 1, 0)), 0, 1)
    activated = jax.nn.silu(layer_norm(attended.astype(jnp.float32), conv_gain)).astype(jnp.bfloat16)

    def finish(pair_in):
        single_act, single_att = pair_in
        convolved = convolve(single_act[None], block_conv)[0]
        return (single_att.astype(jnp.float32) + convolved).astype(jnp.bfloat16)
    return lax.map(finish, (activated, attended))
```

```python
import functools
import math

import jax
import jax.numpy as jnp
import numpy as np
from jax import lax
from jax.experimental import pallas as pl
from jax.experimental.pallas import tpu as pltpu
from jax.sharding import PartitionSpec as P

HEADS = 8
MESH = pl.DeviceIdType.MESH
F32 = jnp.float32
BF16 = jnp.bfloat16


def positions(frame_total, channels):
    frame_pos = np.arange(frame_total, dtype=np.float64)[:, None]
    half_index = np.arange(channels // 2, dtype=np.float64)
    frequency = np.exp(half_index * (-2.0 * math.log(10000.0) / channels))
    angles = frame_pos * frequency
    stacked = np.stack([np.sin(angles), np.cos(angles)], axis=-1)
    return stacked.reshape(frame_total, channels).astype(np.float32)


def norm(values, gain):
    average = jnp.mean(values, axis=-1, keepdims=True)
    centered = values - average
    variance = jnp.mean(centered * centered, axis=-1, keepdims=True)
    return centered * lax.rsqrt(variance + 1e-05) * gain


def silu(values):
    return values / (1.0 + jnp.exp(-values))


def dot(left, right):
    return jnp.dot(left, right, preferred_element_type=F32)


def conv_local(images, weights, sums):
    count, rows, cols, channels = images.shape
    whole = images[...].reshape(-1, channels)
    for b in range(3):
        sums[b] = dot(whole, weights[3 + b]).reshape(count, rows, cols, channels)
    if rows > 1:
        upper = images[:, : rows - 1].reshape(-1, channels)
        lower = images[:, 1:].reshape(-1, channels)
        part = (count, rows - 1, cols, channels)
        for b in range(3):
            sums[b, :, 1:] += dot(upper, weights[b]).reshape(part)
            sums[b, :, : rows - 1] += dot(lower, weights[6 + b]).reshape(part)


def conv_edge(edge, weights, sums, row, taps):
    count, cols, channels = edge.shape
    flat = edge[...].reshape(-1, channels)
    for b in range(3):
        sums[b, :, row] += dot(flat, weights[taps + b]).reshape(count, cols, channels)


def conv_row(sums, index, row):
    left, middle, right = (sums[b, index, row] for b in range(3))
    cols = middle.shape[0]
    col = lax.broadcasted_iota(jnp.int32, middle.shape, 0)
    left = jnp.where(col == 0, 0.0, pltpu.roll(left, 1, 0))
    right = jnp.where(col == cols - 1, 0.0, pltpu.roll(right, cols - 1, 0))
    return left + middle + right


def kernel(
    n,
    row_total,
    lat,
    cond,
    key_frames,
    propagate,
    encoding,
    gain_a,
    gain_c,
    enc_hbm,
    zero_hbm,
    q_hbm,
    k_hbm,
    v_hbm,
    o_hbm,
    blk_hbm,
    out,
    enc_w,
    zero_w,
    q_w,
    k_w,
    v_w,
    o_w,
    blk_w,
    lat_pix,
    keyres,
    res_pix,
    hidden,
    att_pix,
    att,
    act,
    cond_top,
    cond_bot,
    act_top,
    act_bot,
    sums_e,
    sums_b,
    w_sem,
    own_sem,
    lat_send,
    lat_recv,
    res_send,
    res_recv,
    att_send,
    att_recv,
    ch_send,
    ch_recv,
    ah_send,
    ah_recv,
):
    me = lax.axis_index("frame")
    row_me = lax.axis_index("row")
    frames_dev, _, pix, channels = lat.shape
    slots, rows, cols, _ = cond.shape
    frames = frames_dev * n
    head_dim = channels // HEADS
    has_up = row_me > 0
    has_down = row_me < row_total - 1

    pairs = [
        (enc_hbm, enc_w),
        (zero_hbm, zero_w),
        (q_hbm, q_w),
        (k_hbm, k_w),
        (v_hbm, v_w),
        (o_hbm, o_w),
        (blk_hbm, blk_w),
    ]
    loads = [pltpu.make_async_copy(s, d, w_sem.at[i]) for i, (s, d) in enumerate(pairs)]
    for load in loads:
        load.start()

    barrier = pltpu.get_barrier_semaphore()
    for k in range(1, n):
        pl.semaphore_signal(
            barrier, inc=1, device_id={"frame": lax.rem(me + k, n)}, device_id_type=MESH
        )

    @pl.when(has_up)
    def _():
        pl.semaphore_signal(barrier, inc=1, device_id={"row": row_me - 1}, device_id_type=MESH)

    @pl.when(has_down)
    def _():
        pl.semaphore_signal(barrier, inc=1, device_id={"row": row_me + 1}, device_id_type=MESH)

    neighbours = has_up.astype(jnp.int32) + has_down.astype(jnp.int32)
    pl.semaphore_wait(barrier, n - 1 + neighbours)

    def remote(src, dst, send, recv, **where):
        return pltpu.make_async_remote_copy(
            src_ref=src,
            dst_ref=dst,
            send_sem=send,
            recv_sem=recv,
            device_id=where,
            device_id_type=MESH,
        )

    def up(src, dst, send, recv):
        return remote(src, dst, send, recv, row=row_me - 1)

    def down(src, dst, send, recv):
        return remote(src, dst, send, recv, row=row_me + 1)

    cond_up = up(cond.at[:, 0], cond_bot, ch_send.at[0], ch_recv.at[0])
    cond_down = down(cond.at[:, rows - 1], cond_top, ch_send.at[1], ch_recv.at[1])
    pl.when(has_up)(cond_up.start)
    pl.when(has_down)(cond_down.start)

    def spread(src, dst, count, send, recv):
        copies = []
        for k in range(1, n):
            peer = lax.rem(me + k, n)
            copies.append(
                remote(
                    src.at[:, peer],
                    dst.at[pl.ds(me * count, count)],
                    send.at[k],
                    recv.at[k],
                    frame=peer,
                )
            )
        return copies

    lat_copies = spread(lat, lat_pix, frames_dev, lat_send, lat_recv)
    for copy in lat_copies:
        copy.start()
    lat_own = pltpu.make_async_copy(
        lat.at[:, me], lat_pix.at[pl.ds(me * frames_dev, frames_dev)], own_sem.at[0]
    )
    lat_own.start()

    @pl.when(jnp.logical_not(has_up))
    def _():
        cond_top[...] = jnp.zeros_like(cond_top)
        act_top[...] = jnp.zeros_like(act_top)

    @pl.when(jnp.logical_not(has_down))
    def _():
        cond_bot[...] = jnp.zeros_like(cond_bot)
        act_bot[...] = jnp.zeros_like(act_bot)

    loads[0].wait()
    conv_local(cond, enc_w, sums_e)
    pl.when(has_up)(cond_down.wait_recv)
    pl.when(has_down)(cond_up.wait_recv)
    conv_edge(cond_top, enc_w, sums_e, 0, 0)
    conv_edge(cond_bot, enc_w, sums_e, rows - 1, 6)
    loads[1].wait()
    encoded = jnp.concatenate(
        [silu(conv_row(sums_e, s, r)) for s in range(slots) for r in range(rows)], axis=0
    ).astype(BF16)
    keyres[...] = dot(encoded, zero_w[...]).reshape(keyres.shape).astype(BF16)
    res_copies = spread(keyres, res_pix, slots, res_send, res_recv)
    for copy in res_copies:
        copy.start()
    res_own = pltpu.make_async_copy(
        keyres.at[:, me], res_pix.at[pl.ds(me * slots, slots)], own_sem.at[1]
    )
    res_own.start()

    lat_own.wait()
    for copy in lat_copies:
        copy.wait()
    res_own.wait()
    for copy in res_copies:
        copy.wait()

    def hide(f, carry):
        slot = propagate[f]
        gap = jnp.abs(f - key_frames[slot]).astype(F32)
        reach = jnp.exp(jnp.full((1, channels), -gap / (2 * frames_dev), F32))
        value = lat_pix[f].astype(F32) + reach * res_pix[slot].astype(F32)
        hidden[f] = value.astype(BF16).astype(F32)
        return carry

    lax.fori_loop(0, frames, hide, 0, unroll=frames <= 24)

    for load in loads[2:6]:
        load.wait()

    chunk = 16 if pix % 16 == 0 else 8
    group = 8
    block = frames * group
    lane = lax.broadcasted_iota(jnp.int32, (1, channels), 1)
    same = lax.rem(lax.broadcasted_iota(jnp.int32, (block, block), 0), group) == lax.rem(
        lax.broadcasted_iota(jnp.int32, (block, block), 1), group
    )
    scale = 1.0 / math.sqrt(head_dim)
    encode = encoding[...][:, None, :]
    att_copies = []
    for c in range(pix // chunk):
        here = hidden[:, c * chunk : (c + 1) * chunk]
        normed = (norm(here, gain_a[...][None]) + encode).reshape(-1, channels).astype(BF16)
        full = (frames, chunk, channels)
        query = dot(normed, q_w[...]).reshape(full)
        keyp = dot(normed, k_w[...]).reshape(full)
        valp = dot(normed, v_w[...]).reshape(full)
        mixed_parts = []
        for g in range(chunk // group):
            part = slice(g * group, (g + 1) * group)
            q_g = query[:, part].reshape(block, channels).astype(BF16)
            k_g = keyp[:, part].reshape(block, channels).astype(BF16)
            v_g = valp[:, part].reshape(block, channels).astype(BF16)

            def head(h, total):
                mine = (lane >= h * head_dim) & (lane < (h + 1) * head_dim)
                pick = jnp.where(mine, 1.0, 0.0).astype(BF16)
                scores = lax.dot_general(
                    q_g * pick, k_g, (((1,), (1,)), ((), ())), preferred_element_type=F32
                )
                scores = jnp.where(same, scores * scale, -1e30)
                top = jnp.max(scores, axis=-1, keepdims=True)
                powers = jnp.exp(scores - top)
                probs = (powers / jnp.sum(powers, axis=-1, keepdims=True)).astype(BF16)
                return total + dot(probs, v_g * pick)

            zero = jnp.zeros((block, channels), F32)
            mixed = lax.fori_loop(0, HEADS, head, zero, unroll=frames <= 24)
            mixed_parts.append(mixed.reshape(frames, group, channels))
        mixed = jnp.concatenate(mixed_parts, axis=1) if len(mixed_parts) > 1 else mixed_parts[0]
        projected = dot(mixed.reshape(-1, channels).astype(BF16), o_w[...]).reshape(full)
        att_pix[c] = (here + projected).astype(BF16)
        for k in range(1, n):
            peer = lax.rem(me + k, n)
            copy = remote(
                att_pix.at[c, pl.ds(peer * frames_dev, frames_dev)],
                att.at[:, me, c],
                att_send.at[c, k],
                att_recv.at[c, k],
                frame=peer,
            )
            copy.start()
            att_copies.append(copy)
        own = pltpu.make_async_copy(
            att_pix.at[c, pl.ds(me * frames_dev, frames_dev)], att.at[:, me, c], own_sem.at[2 + c]
        )
        own.start()
        att_copies.append(own)
    for copy in att_copies:
        copy.wait()

    act_ups, act_downs = [], []
    for f in range(frames_dev):
        value = att[f].astype(F32).reshape(rows * cols, channels)
        act[f] = silu(norm(value, gain_c[...])).reshape(rows, cols, channels).astype(BF16)
        act_up = up(act.at[f, 0], act_bot.at[f], ah_send.at[0, f], ah_recv.at[0, f])
        act_down = down(act.at[f, rows - 1], act_top.at[f], ah_send.at[1, f], ah_recv.at[1, f])
        pl.when(has_up)(act_up.start)
        pl.when(has_down)(act_down.start)
        act_ups.append(act_up)
        act_downs.append(act_down)

    loads[6].wait()
    conv_local(act, blk_w, sums_b)
    for f in range(frames_dev):
        pl.when(has_up)(act_downs[f].wait_recv)
        pl.when(has_down)(act_ups[f].wait_recv)
    conv_edge(act_top, blk_w, sums_b, 0, 0)
    conv_edge(act_bot, blk_w, sums_b, rows - 1, 6)
    for f in range(frames_dev):
        convolved = jnp.concatenate([conv_row(sums_b, f, r) for r in range(rows)], axis=0)
        value = att[f].astype(F32).reshape(rows * cols, channels)
        out[f] = (value + convolved).reshape(rows, cols, channels).astype(BF16)

    pl.when(has_up)(cond_up.wait_send)
    pl.when(has_down)(cond_down.wait_send)
    for f in range(frames_dev):
        pl.when(has_up)(act_ups[f].wait_send)
        pl.when(has_down)(act_downs[f].wait_send)


def shards(
    latents,
    condition,
    key_frames,
    propagate,
    encoder_conv,
    zero_conv,
    attention_gain,
    query_weight,
    key_weight,
    value_weight,
    output_weight,
    conv_gain,
    block_conv,
):
    frames_dev, rows, cols, channels = latents.shape
    slots = condition.shape[0]
    n = lax.axis_size("frame")
    row_total = lax.axis_size("row")
    pix = rows * cols // n
    frames = frames_dev * n
    chunk = 16 if pix % 16 == 0 else 8
    chunks = pix // chunk
    encoding = jnp.asarray(positions(frames, channels))
    square = (channels, channels)
    vmem = pl.BlockSpec(memory_space=pltpu.VMEM)
    smem = pl.BlockSpec(memory_space=pltpu.SMEM)
    anywhere = pl.BlockSpec(memory_space=pl.ANY)
    dma = pltpu.SemaphoreType.DMA
    return pl.pallas_call(
        functools.partial(kernel, n, row_total),
        out_shape=jax.ShapeDtypeStruct(latents.shape, BF16),
        in_specs=[vmem, vmem, smem, smem, vmem, vmem, vmem] + [anywhere] * 7,
        out_specs=vmem,
        scratch_shapes=[
            pltpu.VMEM((9,) + square, BF16),
            pltpu.VMEM(square, BF16),
            pltpu.VMEM(square, BF16),
            pltpu.VMEM(square, BF16),
            pltpu.VMEM(square, BF16),
            pltpu.VMEM(square, BF16),
            pltpu.VMEM((9,) + square, BF16),
            pltpu.VMEM((frames, pix, channels), BF16),
            pltpu.VMEM((slots, n, pix, channels), BF16),
            pltpu.VMEM((slots * n, pix, channels), BF16),
            pltpu.VMEM((frames, pix, channels), F32),
            pltpu.VMEM((chunks, frames, chunk, channels), BF16),
            pltpu.VMEM((frames_dev, n, chunks, chunk, channels), BF16),
            pltpu.VMEM((frames_dev, rows, cols, channels), BF16),
            pltpu.VMEM((slots, cols, channels), BF16),
            pltpu.VMEM((slots, cols, channels), BF16),
            pltpu.VMEM((frames_dev, cols, channels), BF16),
            pltpu.VMEM((frames_dev, cols, channels), BF16),
            pltpu.VMEM((3, slots, rows, cols, channels), F32),
            pltpu.VMEM((3, frames_dev, rows, cols, channels), F32),
            dma((7,)),
            dma((2 + chunks,)),
            dma((n,)),
            dma((n,)),
            dma((n,)),
            dma((n,)),
            dma((chunks, n)),
            dma((chunks, n)),
            dma((2,)),
            dma((2,)),
            dma((2, frames_dev)),
            dma((2, frames_dev)),
        ],
        compiler_params=pltpu.CompilerParams(
            collective_id=0, has_side_effects=True, vmem_limit_bytes=60 * 1024 * 1024
        ),
    )(
        latents.reshape(frames_dev, n, pix, channels),
        condition,
        key_frames,
        propagate,
        encoding,
        attention_gain.reshape(1, channels),
        conv_gain.reshape(1, channels),
        encoder_conv,
        zero_conv,
        query_weight,
        key_weight,
        value_weight,
        output_weight,
        block_conv,
    )


def solution(mesh):
    placed = (
        P(("group", "frame"), "row", None, None),
        P(("group", "frame"), "row", None, None),
        P("group"),
        P("group"),
        P(),
        P(),
        P(),
        P(),
        P(),
        P(),
        P(),
        P(),
        P(),
    )
    return jax.shard_map(
        shards,
        mesh=mesh,
        in_specs=placed,
        out_specs=P(("group", "frame"), "row", None, None),
        check_vma=False,
    )
```

```python
import functools
import math

import jax
import jax.numpy as jnp
import numpy as np
from jax import lax
from jax.experimental import pallas as pl
from jax.experimental.pallas import tpu as pltpu
from jax.sharding import PartitionSpec as P

HEADS = 8
MESH = pl.DeviceIdType.MESH
F32 = jnp.float32
BF16 = jnp.bfloat16


def positions(frame_total, channels):
    frame_pos = np.arange(frame_total, dtype=np.float64)[:, None]
    half_index = np.arange(channels // 2, dtype=np.float64)
    frequency = np.exp(half_index * (-2.0 * math.log(10000.0) / channels))
    angles = frame_pos * frequency
    stacked = np.stack([np.sin(angles), np.cos(angles)], axis=-1)
    return stacked.reshape(frame_total, channels).astype(np.float32)


def norm(values, gain):
    average = jnp.mean(values, axis=-1, keepdims=True)
    centered = values - average
    variance = jnp.mean(centered * centered, axis=-1, keepdims=True)
    return centered * lax.rsqrt(variance + 1e-05) * gain


def silu(values):
    return values / (1.0 + jnp.exp(-values))


def dot(left, right):
    return jnp.dot(left, right, preferred_element_type=F32)


def flat(values):
    return values.astype(F32).reshape(-1, values.shape[-1]).astype(BF16)


def conv_local(images, weights, sums):
    _, count, rows, cols, channels = sums.shape
    whole = flat(images[...])
    for b in range(3):
        sums[b] = dot(whole, weights[3 + b]).reshape(count, rows, cols, channels)
    if rows > 1:
        upper = flat(images[:, : rows - 1])
        lower = flat(images[:, 1:])
        part = (count, rows - 1, cols, channels)
        for b in range(3):
            sums[b, :, 1:] += dot(upper, weights[b]).reshape(part)
            sums[b, :, : rows - 1] += dot(lower, weights[6 + b]).reshape(part)


def conv_edge(edge, weights, sums, row, taps):
    _, count, _, cols, channels = sums.shape
    values = flat(edge[...])
    for b in range(3):
        sums[b, :, row] += dot(values, weights[taps + b]).reshape(count, cols, channels)


def conv_row(sums, index, row):
    left, middle, right = (sums[b, index, row] for b in range(3))
    cols = middle.shape[0]
    col = lax.broadcasted_iota(jnp.int32, middle.shape, 0)
    left = jnp.where(col == 0, 0.0, pltpu.roll(left, 1, 0))
    right = jnp.where(col == cols - 1, 0.0, pltpu.roll(right, cols - 1, 0))
    return left + middle + right


def kernel(
    n,
    row_total,
    lat,
    cond_hbm,
    key_frames,
    propagate,
    encoding,
    gain_a,
    gain_c,
    enc_hbm,
    zero_hbm,
    q_hbm,
    k_hbm,
    v_hbm,
    o_hbm,
    blk_hbm,
    out,
    cond,
    enc_w,
    zero_w,
    q_w,
    k_w,
    v_w,
    o_w,
    blk_w,
    lat_pix,
    keyres,
    res_pix,
    hidden,
    att_pix,
    att,
    act,
    cond_top,
    cond_bot,
    act_top,
    act_bot,
    sums_e,
    sums_b,
    w_sem,
    own_sem,
    lat_send,
    lat_recv,
    res_send,
    res_recv,
    att_send,
    att_recv,
    ch_send,
    ch_recv,
    ah_send,
    ah_recv,
):
    me = lax.axis_index("frame")
    row_me = lax.axis_index("row")
    frames_dev, _, pix, channels = lat.shape
    slots, rows, cols, _ = cond.shape
    chunks = res_recv.shape[0]
    chunk = pix // chunks
    group = att.shape[3]
    per_chunk = chunk // group
    frames = frames_dev * n
    head_dim = channels // HEADS
    has_up = row_me > 0
    has_down = row_me < row_total - 1

    pairs = [
        (cond_hbm, cond),
        (enc_hbm, enc_w),
        (zero_hbm, zero_w),
        (q_hbm, q_w),
        (k_hbm, k_w),
        (v_hbm, v_w),
        (o_hbm, o_w),
        (blk_hbm, blk_w),
    ]
    loads = [pltpu.make_async_copy(s, d, w_sem.at[i]) for i, (s, d) in enumerate(pairs)]
    for load in loads:
        load.start()

    barrier = pltpu.get_barrier_semaphore()
    for k in range(1, n):
        pl.semaphore_signal(
            barrier, inc=1, device_id={"frame": lax.rem(me + k, n)}, device_id_type=MESH
        )

    @pl.when(has_up)
    def _():
        pl.semaphore_signal(barrier, inc=1, device_id={"row": row_me - 1}, device_id_type=MESH)

    @pl.when(has_down)
    def _():
        pl.semaphore_signal(barrier, inc=1, device_id={"row": row_me + 1}, device_id_type=MESH)

    neighbours = has_up.astype(jnp.int32) + has_down.astype(jnp.int32)
    pl.semaphore_wait(barrier, n - 1 + neighbours)

    def remote(src, dst, send, recv, **where):
        return pltpu.make_async_remote_copy(
            src_ref=src,
            dst_ref=dst,
            send_sem=send,
            recv_sem=recv,
            device_id=where,
            device_id_type=MESH,
        )

    def up(src, dst, send, recv):
        return remote(src, dst, send, recv, row=row_me - 1)

    def down(src, dst, send, recv):
        return remote(src, dst, send, recv, row=row_me + 1)

    cond_up = up(cond_hbm.at[:, 0], cond_bot, ch_send.at[0], ch_recv.at[0])
    cond_down = down(cond_hbm.at[:, rows - 1], cond_top, ch_send.at[1], ch_recv.at[1])
    pl.when(has_up)(cond_up.start)
    pl.when(has_down)(cond_down.start)

    def spread(src, dst, count, send, recv):
        copies = []
        for k in range(1, n):
            peer = lax.rem(me + k, n)
            copies.append(
                remote(
                    src.at[:, peer],
                    dst.at[pl.ds(me * count, count)],
                    send.at[k],
                    recv.at[k],
                    frame=peer,
                )
            )
        return copies

    lat_copies = spread(lat, lat_pix, frames_dev, lat_send, lat_recv)
    for copy in lat_copies:
        copy.start()
    lat_own = pltpu.make_async_copy(
        lat.at[:, me], lat_pix.at[pl.ds(me * frames_dev, frames_dev)], own_sem.at[0]
    )
    lat_own.start()

    @pl.when(jnp.logical_not(has_up))
    def _():
        cond_top[...] = jnp.zeros_like(cond_top)
        act_top[...] = jnp.zeros_like(act_top)

    @pl.when(jnp.logical_not(has_down))
    def _():
        cond_bot[...] = jnp.zeros_like(cond_bot)
        act_bot[...] = jnp.zeros_like(act_bot)

    loads[0].wait()
    loads[1].wait()
    conv_local(cond, enc_w, sums_e)
    pl.when(has_up)(cond_down.wait_recv)
    pl.when(has_down)(cond_up.wait_recv)
    conv_edge(cond_top, enc_w, sums_e, 0, 0)
    conv_edge(cond_bot, enc_w, sums_e, rows - 1, 6)
    loads[2].wait()
    encoded = jnp.concatenate(
        [silu(conv_row(sums_e, s, r)) for s in range(slots) for r in range(rows)], axis=0
    ).astype(BF16)
    keyres[...] = dot(encoded, zero_w[...]).reshape(keyres.shape).astype(BF16)
    res_copies = []
    for c in range(chunks):
        span = pl.ds(c * chunk, chunk)
        for k in range(1, n):
            peer = lax.rem(me + k, n)
            copy = remote(
                keyres.at[:, peer, span],
                res_pix[c].at[pl.ds(me * slots, slots)],
                res_send.at[c, k],
                res_recv.at[c, k],
                frame=peer,
            )
            copy.start()
            res_copies.append(copy)
        own = pltpu.make_async_copy(
            keyres.at[:, me, span], res_pix[c].at[pl.ds(me * slots, slots)], own_sem.at[1 + c]
        )
        own.start()
        res_copies.append(own)

    lat_own.wait()
    for copy in lat_copies:
        copy.wait()

    for load in loads[3:7]:
        load.wait()

    small = frames <= 24
    block = frames * group
    same = lax.rem(lax.broadcasted_iota(jnp.int32, (block, block), 0), group) == lax.rem(
        lax.broadcasted_iota(jnp.int32, (block, block), 1), group
    )
    scale = 1.0 / math.sqrt(head_dim)
    encode = encoding[...][:, None, :]

    def head(h, start, queries, keys, values):
        lane = start + lax.broadcasted_iota(jnp.int32, (1, queries.shape[1]), 1)
        mine = (lane >= h * head_dim) & (lane < (h + 1) * head_dim)
        pick = jnp.where(mine, 1.0, 0.0).astype(BF16)
        scores = lax.dot_general(
            queries * pick, keys, (((1,), (1,)), ((), ())), preferred_element_type=F32
        )
        scores = jnp.where(same, scores * scale, -1e30)
        top = jnp.max(scores, axis=-1, keepdims=True)
        powers = jnp.exp(scores - top)
        probs = (powers / jnp.sum(powers, axis=-1, keepdims=True)).astype(BF16)
        return dot(probs, values * pick)

    def windows(h):
        start = -(-max(0, (h + 1) * head_dim - 256) // 128) * 128
        return start, min(start + 256, channels)

    def attend(queries, keys, values):
        if not small or head_dim > 128:
            return lax.fori_loop(
                0,
                HEADS,
                lambda h, total: total + head(h, 0, queries, keys, values),
                jnp.zeros((block, channels), F32),
            )
        totals = {}
        for h in range(HEADS):
            start, stop = windows(h)
            cut = slice(start, stop)
            mixed = head(h, start, queries[:, cut], keys[:, cut], values[:, cut])
            totals[start] = mixed if start not in totals else totals[start] + mixed
        tiles = []
        for low in range(0, channels, 128):
            high = min(low + 128, channels)
            held = [
                value[:, low - start : high - start]
                for start, value in totals.items()
                if start <= low and high <= start + value.shape[1]
            ]
            tiles.append(sum(held[1:], held[0]))
        return jnp.concatenate(tiles, axis=1)

    att_copies = []
    for c in range(chunks):
        span = slice(c * chunk, (c + 1) * chunk)
        for copy in res_copies[c * n : (c + 1) * n]:
            copy.wait()

        def hide(f, carry):
            slot = propagate[f]
            gap = jnp.abs(f - key_frames[slot]).astype(F32)
            reach = jnp.exp(jnp.full((1, channels), -gap / (2 * frames_dev), F32))
            value = lat_pix[f, span].astype(F32) + reach * res_pix[c][slot].astype(F32)
            hidden[f, span] = value.astype(BF16).astype(F32)
            return carry

        lax.fori_loop(0, frames, hide, 0, unroll=small)
        here = hidden[:, span]
        normed = (norm(here, gain_a[...]) + encode).reshape(-1, channels).astype(BF16)
        full = (frames, chunk, channels)
        query = dot(normed, q_w[...]).reshape(full)
        keyp = dot(normed, k_w[...]).reshape(full)
        valp = dot(normed, v_w[...]).reshape(full)
        for g in range(per_chunk):
            s = c * per_chunk + g
            part = slice(g * group, (g + 1) * group)
            mixed = attend(
                query[:, part].reshape(block, channels).astype(BF16),
                keyp[:, part].reshape(block, channels).astype(BF16),
                valp[:, part].reshape(block, channels).astype(BF16),
            )
            projected = dot(mixed.astype(BF16), o_w[...]).reshape(frames, group, channels)
            base = hidden[:, s * group : (s + 1) * group]
            att_pix[s] = (base + projected).astype(BF16)
            for k in range(1, n):
                peer = lax.rem(me + k, n)
                copy = remote(
                    att_pix.at[s, pl.ds(peer * frames_dev, frames_dev)],
                    att.at[:, me, s],
                    att_send.at[s, k],
                    att_recv.at[s, k],
                    frame=peer,
                )
                copy.start()
                att_copies.append(copy)
            own = pltpu.make_async_copy(
                att_pix.at[s, pl.ds(me * frames_dev, frames_dev)],
                att.at[:, me, s],
                own_sem.at[1 + chunks + s],
            )
            own.start()
            att_copies.append(own)

    pieces = chunks * per_chunk
    piece = (frames_dev, rows, n // rows, group, channels)
    act_ups, act_downs = [], []
    for s in range(pieces):
        for copy in att_copies[s * n : (s + 1) * n]:
            copy.wait()
        value = att[:, :, s].astype(F32)
        act[:, :, :, s] = silu(norm(value, gain_c[...])).astype(BF16).reshape(piece)
        act_up = up(act.at[:, 0, :, s], act_bot.at[:, :, s], ah_send.at[0, s], ah_recv.at[0, s])
        act_down = down(
            act.at[:, rows - 1, :, s], act_top.at[:, :, s], ah_send.at[1, s], ah_recv.at[1, s]
        )
        pl.when(has_up)(act_up.start)
        pl.when(has_down)(act_down.start)
        act_ups.append(act_up)
        act_downs.append(act_down)

    loads[7].wait()
    conv_local(act, blk_w, sums_b)
    for s in range(pieces):
        pl.when(has_up)(act_downs[s].wait_recv)
        pl.when(has_down)(act_ups[s].wait_recv)
    conv_edge(act_top, blk_w, sums_b, 0, 0)
    conv_edge(act_bot, blk_w, sums_b, rows - 1, 6)
    for f in range(frames_dev):
        convolved = jnp.concatenate([conv_row(sums_b, f, r) for r in range(rows)], axis=0)
        value = att[f].astype(F32).reshape(rows * cols, channels)
        out[f] = (value + convolved).reshape(rows, cols, channels).astype(BF16)

    pl.when(has_up)(cond_up.wait_send)
    pl.when(has_down)(cond_down.wait_send)
    for s in range(pieces):
        pl.when(has_up)(act_ups[s].wait_send)
        pl.when(has_down)(act_downs[s].wait_send)


def shards(
    latents,
    condition,
    key_frames,
    propagate,
    encoder_conv,
    zero_conv,
    attention_gain,
    query_weight,
    key_weight,
    value_weight,
    output_weight,
    conv_gain,
    block_conv,
):
    frames_dev, rows, cols, channels = latents.shape
    slots = condition.shape[0]
    n = lax.axis_size("frame")
    row_total = lax.axis_size("row")
    pix = rows * cols // n
    frames = frames_dev * n
    chunk = 16 if pix % 16 == 0 else 8
    chunks = pix // chunk
    group = 8
    pieces = pix // group
    per_row = n // rows
    encoding = jnp.asarray(positions(frames, channels))
    square = (channels, channels)
    vmem = pl.BlockSpec(memory_space=pltpu.VMEM)
    smem = pl.BlockSpec(memory_space=pltpu.SMEM)
    anywhere = pl.BlockSpec(memory_space=pl.ANY)
    dma = pltpu.SemaphoreType.DMA
    return pl.pallas_call(
        functools.partial(kernel, n, row_total),
        out_shape=jax.ShapeDtypeStruct(latents.shape, BF16),
        in_specs=[anywhere, anywhere, smem, smem, vmem, vmem, vmem] + [anywhere] * 7,
        out_specs=vmem,
        scratch_shapes=[
            pltpu.VMEM(condition.shape, BF16),
            pltpu.VMEM((9,) + square, BF16),
            pltpu.VMEM(square, BF16),
            pltpu.VMEM(square, BF16),
            pltpu.VMEM(square, BF16),
            pltpu.VMEM(square, BF16),
            pltpu.VMEM(square, BF16),
            pltpu.VMEM((9,) + square, BF16),
            pltpu.VMEM((frames, pix, channels), BF16),
            pltpu.VMEM((slots, n, pix, channels), BF16),
            [pltpu.VMEM((slots * n, chunk, channels), BF16) for _ in range(chunks)],
            pltpu.VMEM((frames, pix, channels), F32),
            pltpu.VMEM((pieces, frames, group, channels), BF16),
            pltpu.VMEM((frames_dev, n, pieces, group, channels), BF16),
            pltpu.VMEM((frames_dev, rows, per_row, pieces, group, channels), BF16),
            pltpu.VMEM((slots, cols, channels), BF16),
            pltpu.VMEM((slots, cols, channels), BF16),
            pltpu.VMEM((frames_dev, per_row, pieces, group, channels), BF16),
            pltpu.VMEM((frames_dev, per_row, pieces, group, channels), BF16),
            pltpu.VMEM((3, slots, rows, cols, channels), F32),
            pltpu.VMEM((3, frames_dev, rows, cols, channels), F32),
            dma((8,)),
            dma((1 + chunks + pieces,)),
            dma((n,)),
            dma((n,)),
            dma((chunks, n)),
            dma((chunks, n)),
            dma((pieces, n)),
            dma((pieces, n)),
            dma((2,)),
            dma((2,)),
            dma((2, pieces)),
            dma((2, pieces)),
        ],
        compiler_params=pltpu.CompilerParams(
            collective_id=0, has_side_effects=True, vmem_limit_bytes=60 * 1024 * 1024
        ),
    )(
        latents.reshape(frames_dev, n, pix, channels),
        condition,
        key_frames,
        propagate,
        encoding,
        attention_gain,
        conv_gain,
        encoder_conv,
        zero_conv,
        query_weight,
        key_weight,
        value_weight,
        output_weight,
        block_conv,
    )


def solution(mesh):
    placed = (
        P(("group", "frame"), "row", None, None),
        P(("group", "frame"), "row", None, None),
        P("group"),
        P("group"),
        P(),
        P(),
        P(),
        P(),
        P(),
        P(),
        P(),
        P(),
        P(),
    )
    return jax.shard_map(
        shards,
        mesh=mesh,
        in_specs=placed,
        out_specs=P(("group", "frame"), "row", None, None),
        check_vma=False,
    )
```
